32 devices in a mesh: leaf: 8 (over z, x), vec: 4 (over y, core).
Axes of the slice: x: 2, y: 2, z: 4, core: 2. Of those that a mesh axis runs over, the one named last changes fastest.
Arguments:
- samples: bfloat16 [64, 32768], P('vec', 'leaf'), may hold values from -6 to 6
- coords: float32 [3, 32768], P(None, 'leaf'), may hold values from -4 to 4
- panel_area: float32 [32768], P('leaf'), may hold values from 0.05 to 0.5
- quad_weight: float32 [32768], P('leaf'), may hold values from 0.2 to 1
- leaf_basis: bfloat16 [128, 64, 256], P('leaf'), may hold values from -0.375 to 0.375
- transfer: bfloat16 [64, 2, 64, 64], P('leaf'), may hold values from -0.5 to 0.5
- coupling_fine: bfloat16 [128, 16, 64, 64], P('leaf'), may hold values from -0.1875 to 0.1875
- coupling_coarse: bfloat16 [64, 16, 64, 64], P('leaf'), may hold values from -0.1875 to 0.1875
- near_list: int32 [128, 16], P('leaf'), may hold values from 0 to 127, as said below
- send_fine: int32 [64, 32], P('leaf'), may hold values from 0 to 15
- send_coarse: int32 [64, 16], P('leaf'), may hold values from 0 to 7
- far_fine: int32 [128, 16], P('leaf'), may hold values from 0 to 255, as said below
- far_coarse: int32 [64, 16], P('leaf'), may hold values from 0 to 127, as said below
Outputs:
- sample_out: bfloat16 [64, 32768], P('vec', 'leaf')
- sample_gram: float32 [128, 64, 64], P('leaf', 'vec')
The draws below stay inside these ranges and needn't reach their ends.
Inputs may be any that keep to these rules, and one draw needn't show every extreme that they name: `near_list`: row g names 16 different leaves, each at most 16 leaves from g. `send_fine`: row e * 8 + d names clusters of device e, counted on e from 0; every slot carries one. `send_coarse`: row e * 8 + d names clusters of device e, counted on e from 0; every slot carries one. `far_fine`: the rows of one device's 16 leaves name each of the values 0 to 255 exactly once. `far_coarse`: the rows of one device's parents name each of the values 0 to 127 exactly once.
All inputs are finite; a program needn't handle non-finite values.
Results may differ from the reference program's by a relative error of at most 0.0085.
Values may be sent and summed in bfloat16 or wider, within the bound.
A program may use at most 64 MiB of HBM per device.

```python
import math
import jax
import jax.numpy as jnp
from jax import lax

LEAF = 256
K = 64
VECS = 64
NN = 16
HW = 16
NB = 16
LEAF_DEV = 16
LEAVES = 128
POINTS = 32768
PARENTS = 64
CAP0 = 32
CAP1 = 16
N_LEAF = 8


def draw_near_list(key, part):
    window_len = 2 * HW + 1
    offsets = jnp.arange(window_len, dtype=jnp.int32) - HW
    rank_bits = jax.random.randint(key, (LEAVES, window_len), 0, 1 << 20, dtype=jnp.int32)
    owner_leaf = jnp.arange(LEAVES, dtype=jnp.int32)[:, None]
    target = owner_leaf + offsets[None, :]
    inside = (target >= 0) & (target < LEAVES)
    scores = jnp.where(inside, rank_bits + (1 << 20), 0) * window_len + jnp.arange(window_len, dtype=jnp.int32)[None, :]
    top_scores, picked = lax.top_k(scores, NN)
    return jnp.take_along_axis(target, picked, axis=1).astype(jnp.int32)


def permuted_rows(key, per_device, width_nb):
    devices = LEAVES // LEAF_DEV
    device_keys = jax.random.split(key, devices)
    permuted = jax.vmap(lambda subkey: jax.random.permutation(subkey, per_device * width_nb))(device_keys)
    return permuted.reshape(devices * per_device, width_nb).astype(jnp.int32)


def draw_far_fine(key, part):
    return permuted_rows(jax.random.fold_in(key, 11), LEAF_DEV, NB)


def draw_far_coarse(key, part):
    return permuted_rows(jax.random.fold_in(key, 23), LEAF_DEV // 2, NB)


def touch_ends(values, key, least, largest):
    extent = values.shape
    place = [jax.random.randint(jax.random.fold_in(key, axis), (), 0, extent[axis]) for axis in range(len(extent))]
    values = values.at[tuple(place)].set(least)
    longest = extent.index(max(extent))
    place[longest] = (place[longest] + 1) % extent[longest]
    return values.at[tuple(place)].set(largest)


def block_levels(own_key, dims, cuts, least, largest):
    loudness, own = 1.0, jax.random.fold_in(own_key, 6)
    for dim, shards_of in cuts:
        steps = jnp.exp(jax.random.uniform(jax.random.fold_in(own, dim), (shards_of,), jnp.float32, least / len(cuts), largest / len(cuts)))
        loudness = loudness * jnp.repeat(steps, dims[dim] // shards_of).reshape([-1 if axis == dim else 1 for axis in range(len(dims))])
    return loudness


def centred(stream_key, shape, width, reach, pieces=(), held_as=jnp.bfloat16):
    result = width * jax.random.normal(stream_key, shape, jnp.float32)
    if pieces:
        result = result * block_levels(stream_key, shape, pieces, -0.22, 0.18)
    return jnp.clip(result, -reach, reach).astype(held_as)


def setup_inputs(seed: int = 0) -> dict:
    splits = jax.random.split(jax.random.key(seed), 14)
    return {
        "samples": centred(splits[0], (VECS, POINTS), 1.0, 6.0, ((0, 4), (1, 8))),
        "coords": centred(splits[1], (3, POINTS), 0.3, 4.0, ((1, 8),), jnp.float32),
        "panel_area": jnp.clip(jnp.exp(math.log(0.5) - 2.3025851 * jax.random.uniform(splits[2], (POINTS,), jnp.float32) ** block_levels(splits[2], (POINTS,), ((0, 8),), -0.2, 0.2)), 0.05, 0.5),
        "quad_weight": jnp.clip(0.2 + 0.8 * jax.random.uniform(splits[3], (POINTS,), jnp.float32) ** block_levels(splits[3], (POINTS,), ((0, 8),), -0.2, 0.2), 0.2, 1.0),
        "leaf_basis": centred(splits[4], (LEAVES, K, LEAF), LEAF ** -0.5, 0.375, ((0, 8),)),
        "transfer": centred(splits[5], (PARENTS, 2, K, K), (2 * K) ** -0.5, 0.5, ((0, 8),)),
        "coupling_fine": centred(splits[6], (LEAVES, NB, K, K), (NB * K) ** -0.5, 0.1875, ((0, 8),)),
        "coupling_coarse": centred(splits[7], (PARENTS, NB, K, K), (NB * K) ** -0.5, 0.1875, ((0, 8),)),
        "near_list": draw_near_list(jax.random.fold_in(splits[13], 71), 0),
        "send_fine": touch_ends(jax.random.randint(splits[9], (N_LEAF * N_LEAF, CAP0), 0, LEAF_DEV), jax.random.fold_in(splits[9], 1), 0, LEAF_DEV - 1).astype(jnp.int32),
        "send_coarse": touch_ends(jax.random.randint(splits[10], (N_LEAF * N_LEAF, CAP1), 0, LEAF_DEV // 2), jax.random.fold_in(splits[10], 1), 0, (LEAF_DEV // 2) - 1).astype(jnp.int32),
        "far_fine": draw_far_fine(jax.random.fold_in(splits[13], 71), 0),
        "far_coarse": draw_far_coarse(jax.random.fold_in(splits[13], 71), 0),
    }


four_pi = 4.0 * 3.141592653589793

def kernel_block(target, source):
    delta_x = target[0][:, None] - source[0][None, :]
    delta_y = target[1][:, None] - source[1][None, :]
    delta_z = target[2][:, None] - source[2][None, :]
    distance = delta_x * delta_x + delta_y * delta_y + delta_z * delta_z + source[3][None, :]
    return (source[4][None, :] / (four_pi * jnp.sqrt(distance))).astype(jnp.bfloat16)

def near_field(samples, geometry, near_list):
    leaves = near_list.shape[0]
    geo_all = geometry.reshape(5, leaves, LEAF)
    values = samples.reshape(samples.shape[0], leaves, LEAF)

    def leaf_group(indices):

        def one_leaf(index):
            chosen = near_list[index]
            src_geo = jnp.take(geo_all, chosen, axis=1)
            src_val = jnp.take(values, chosen, axis=1).astype(jnp.float32)
            target = jnp.take(geo_all[:3], index, axis=1)
            blocks = jax.vmap(kernel_block, (None, 1))(target, src_geo)
            return jnp.einsum('npq,vnq->vp', blocks.astype(jnp.float32), src_val)
        return jax.vmap(one_leaf)(indices)
    results = lax.map(leaf_group, jnp.arange(leaves, dtype=jnp.int32).reshape(-1, 8))
    return results.reshape(leaves, samples.shape[0], LEAF)

def partner_map(far_list, send_plan, per_device):
    slots = send_plan.shape[1]
    devices = far_list.shape[0] // per_device
    owner_dev = (jnp.arange(far_list.shape[0], dtype=jnp.int32) // per_device)[:, None]
    source = far_list // slots
    slot_index = far_list % slots
    local_index = send_plan[source * devices + owner_dev, slot_index]
    return (source * per_device + local_index).astype(jnp.int32)

def couple(tile_set, coef_table, partners, per_device):
    devices = partners.shape[0] // per_device
    width_nb = partners.shape[1]
    tile_set = tile_set.reshape(devices, per_device, width_nb, K, K)
    partners = partners.reshape(devices, per_device, width_nb)

    def one_device(operands):
        tiles, chosen = operands
        picked = coef_table[chosen].astype(jnp.float32)
        return jnp.einsum('ibkl,ibvl->ivk', tiles.astype(jnp.float32), picked)
    results = lax.map(one_device, (tile_set, partners))
    return results.reshape(devices * per_device, coef_table.shape[1], K)

def reference(samples, coords, panel_area, quad_weight, leaf_basis, transfer, coupling_fine, coupling_coarse, near_list, send_fine, send_coarse, far_fine, far_coarse):
    vectors = samples.shape[0]
    leaves = leaf_basis.shape[0]
    geometry = jnp.concatenate([coords, panel_area[None, :], quad_weight[None, :]], axis=0)
    near_part = near_field(samples, geometry, near_list)
    local_rows = samples.reshape(vectors, leaves, LEAF).astype(jnp.float32)
    fine_coef = jnp.einsum('ikp,vip->ivk', leaf_basis.astype(jnp.float32), local_rows).astype(jnp.bfloat16)
    coarse_coef = jnp.einsum('mskl,msvk->mvl', transfer.astype(jnp.float32), fine_coef.reshape(-1, 2, vectors, K).astype(jnp.float32)).astype(jnp.bfloat16)
    fine_partners = partner_map(far_fine, send_fine, LEAF_DEV)
    coarse_partners = partner_map(far_coarse, send_coarse, LEAF_DEV // 2)
    field_fine = couple(coupling_fine, fine_coef, fine_partners, LEAF_DEV)
    field_coarse = couple(coupling_coarse, coarse_coef, coarse_partners, LEAF_DEV // 2).astype(jnp.bfloat16)
    pushed = jnp.einsum('mskl,mvl->msvk', transfer.astype(jnp.float32), field_coarse.astype(jnp.float32))
    local_field = (field_fine + pushed.reshape(leaves, vectors, K)).astype(jnp.bfloat16)
    far_part = jnp.einsum('ikp,ivk->vip', leaf_basis.astype(jnp.float32), local_field.astype(jnp.float32))
    sample_out = (jnp.transpose(near_part, (1, 0, 2)) + far_part).reshape(vectors, leaves * LEAF).astype(jnp.bfloat16)
    shaped = sample_out.reshape(vectors, leaves, LEAF).astype(jnp.float32)
    sample_gram = jnp.einsum('aip,cip->iac', shaped, shaped) * (1.0 / LEAF)
    return (sample_out, sample_gram)
```

```python
import functools
import jax
import jax.numpy as jnp
from jax import lax
from jax.experimental import pallas as pl
from jax.experimental.pallas import tpu as pltpu
from jax.sharding import PartitionSpec as P

four_pi = 4.0 * 3.141592653589793
NT = (((1,), (1,)), ((), ()))


def pieces(block):
    first = block.astype(jnp.bfloat16).astype(jnp.float32)
    rest = block - first
    second = rest.astype(jnp.bfloat16).astype(jnp.float32)
    return first, second, rest - second


def main_kernel(
    devices, leaf_dev, leaf_pts, cap0, cap1,
    near_ref, farf_ref, farc_ref, sendf_ref, sendc_ref,
    geo_ref, vec_ref, fine_ref, coarse_ref, cf_ref, cc_ref, transfer_ref, basis_ref,
    out_ref, yfeat, xfeat,
):
    parents = leaf_dev // 2
    nb = farf_ref.shape[0] // leaf_dev
    nbc = farc_ref.shape[0] // parents
    nn = near_ref.shape[0] // leaf_dev

    def make_source(leaf, carry):
        y1, y2, y3 = pieces(geo_ref[leaf])
        rows = jnp.concatenate([y1, y1, y1, y2, y2, y3], axis=0)
        yfeat[leaf] = rows.T.astype(jnp.bfloat16)
        return carry

    lax.fori_loop(0, 3 * leaf_dev, make_source, 0)

    def make_target(leaf, carry):
        geo = geo_ref[leaf_dev + leaf]
        xyz = geo[0:3]
        norm = jnp.sum(xyz * xyz, axis=0, keepdims=True)
        one = jnp.ones_like(norm)
        x8 = jnp.concatenate([-2.0 * xyz, one, norm, jnp.zeros_like(xyz)], axis=0)
        x1, x2, x3 = pieces(x8)
        xfeat[leaf] = jnp.concatenate([x1, x2, x3, x1, x2, x1], axis=0).astype(jnp.bfloat16)
        return carry

    lax.fori_loop(0, leaf_dev, make_target, 0)

    def near_sum(leaf):
        target = xfeat[leaf]

        def step(group, total):
            for lane in range(4):
                chosen = near_ref[leaf * nn + group * 4 + lane]
                dist = jnp.dot(yfeat[chosen], target, preferred_element_type=jnp.float32)
                block = lax.rsqrt(dist.astype(jnp.bfloat16))
                total = total + jnp.dot(vec_ref[chosen], block, preferred_element_type=jnp.float32)
            return total

        zero = jnp.zeros((vec_ref.shape[1], leaf_pts), jnp.float32)
        return lax.fori_loop(0, nn // 4, step, zero)

    def nt(a, b):
        return lax.dot_general(a, b, NT, preferred_element_type=jnp.float32)

    def parent(m, carry):
        coarse = None
        for b in range(nbc):
            row = farc_ref[m * nbc + b]
            src = (row // cap1) * parents + sendc_ref[row]
            term = nt(coarse_ref[src], cc_ref[m, b])
            coarse = term if coarse is None else coarse + term
        coarse = coarse.astype(jnp.bfloat16)
        for s in range(2):
            leaf = 2 * m + s
            field = nt(coarse, transfer_ref[m, s])
            for b in range(nb):
                row = farf_ref[leaf * nb + b]
                src = (row // cap0) * leaf_dev + sendf_ref[row]
                field = field + nt(fine_ref[src], cf_ref[leaf, b])
            local = field.astype(jnp.bfloat16)
            far = jnp.dot(local, basis_ref[leaf], preferred_element_type=jnp.float32)
            out_ref[leaf] = (near_sum(leaf) + far).astype(out_ref.dtype)
        return carry

    lax.fori_loop(0, parents, parent, 0)


def per_device(
    samples, coords, panel_area, quad_weight, leaf_basis, transfer,
    coupling_fine, coupling_coarse, near_list, send_fine, send_coarse, far_fine, far_coarse,
):
    vec_dev, points = samples.shape
    leaf_dev, basis_rank, leaf_pts = leaf_basis.shape
    devices = lax.axis_size("leaf")
    device = lax.axis_index("leaf")
    cap0, cap1 = send_fine.shape[1], send_coarse.shape[1]
    norm = jnp.sum(coords * coords, axis=0, keepdims=True) + panel_area[None, :]
    geo = jnp.concatenate(
        [coords, norm, jnp.ones_like(norm), jnp.zeros_like(coords)], axis=0
    ).reshape(8, leaf_dev, leaf_pts).transpose(1, 0, 2)
    weighted = (samples.astype(jnp.float32) * (quad_weight / four_pi)[None, :]).astype(jnp.bfloat16)
    weighted = weighted.reshape(vec_dev, leaf_dev, leaf_pts).transpose(1, 0, 2)
    forward = [(i, i + 1) for i in range(devices - 1)]
    backward = [(i + 1, i) for i in range(devices - 1)]

    def wide(block):
        low = lax.ppermute(block, "leaf", forward)
        high = lax.ppermute(block, "leaf", backward)
        return jnp.concatenate([low, block, high], axis=0)

    geo_wide, vec_wide = wide(geo), wide(weighted)
    window = (near_list - (device * leaf_dev - leaf_dev)).reshape(-1)
    rows = samples.reshape(vec_dev, leaf_dev, leaf_pts)
    fine_coef = jnp.einsum(
        "ikp,vip->ivk", leaf_basis, rows, preferred_element_type=jnp.float32
    ).astype(jnp.bfloat16)
    coarse_coef = jnp.einsum(
        "mskl,msvk->mvl",
        transfer,
        fine_coef.reshape(-1, 2, vec_dev, basis_rank),
        preferred_element_type=jnp.float32,
    ).astype(jnp.bfloat16)
    fine_all = lax.all_gather(fine_coef, "leaf", axis=0, tiled=True)
    coarse_all = lax.all_gather(coarse_coef, "leaf", axis=0, tiled=True)
    send = jnp.concatenate([send_fine, send_coarse], axis=1)
    got = lax.all_to_all(send, "leaf", split_axis=0, concat_axis=0, tiled=True)
    smem = pl.BlockSpec(memory_space=pltpu.SMEM)
    vmem = pl.BlockSpec(memory_space=pltpu.VMEM)
    out = pl.pallas_call(
        functools.partial(main_kernel, devices, leaf_dev, leaf_pts, cap0, cap1),
        out_shape=jax.ShapeDtypeStruct((leaf_dev, vec_dev, leaf_pts), jnp.bfloat16),
        in_specs=[smem] * 5 + [vmem] * 8,
        out_specs=vmem,
        scratch_shapes=[
            pltpu.VMEM((3 * leaf_dev, leaf_pts, 48), jnp.bfloat16),
            pltpu.VMEM((leaf_dev, 48, leaf_pts), jnp.bfloat16),
        ],
        compiler_params=pltpu.CompilerParams(vmem_limit_bytes=56 * 1024 * 1024),
    )(
        window, far_fine.reshape(-1), far_coarse.reshape(-1),
        got[:, :cap0].reshape(-1), got[:, cap0:].reshape(-1),
        geo_wide, vec_wide, fine_all, coarse_all, coupling_fine, coupling_coarse, transfer, leaf_basis,
    )
    gathered = lax.all_gather(out, "vec", axis=1, tiled=True)
    gram = jnp.einsum("ivp,iwp->ivw", out, gathered, preferred_element_type=jnp.float32)
    gram = gram * (1.0 / leaf_pts)
    sample_out = out.transpose(1, 0, 2).reshape(vec_dev, points)
    return sample_out, gram


def solution(mesh):
    return jax.shard_map(
        per_device,
        mesh=mesh,
        in_specs=(
            P("vec", "leaf"), P(None, "leaf"), P("leaf"), P("leaf"),
            P("leaf", None, None), P("leaf", None, None, None),
            P("leaf", None, None, None), P("leaf", None, None, None),
            P("leaf", None), P("leaf", None), P("leaf", None), P("leaf", None), P("leaf", None),
        ),
        out_specs=(P("vec", "leaf"), P("leaf", "vec", None)),
        check_vma=False,
    )
```

```python
import functools
import jax
import jax.numpy as jnp
from jax import lax
from jax.experimental import pallas as pl
from jax.experimental.pallas import tpu as pltpu
from jax.sharding import PartitionSpec as P

four_pi = 4.0 * 3.141592653589793
NT = (((1,), (1,)), ((), ()))
MESH = pl.DeviceIdType.MESH


def pieces(block):
    first = block.astype(jnp.bfloat16).astype(jnp.float32)
    rest = block - first
    second = rest.astype(jnp.bfloat16).astype(jnp.float32)
    return first, second, rest - second


def main_kernel(
    near_ref, farf_ref, farc_ref,
    geo_ref, sam_ref, send_ref, transfer_ref, basis_ref, cf_hbm, cc_hbm,
    out_ref, gram_ref,
    geo_low, geo_high, sam_low, sam_high, fine_all, coarse_all, got, got_smem, cf_ref, cc_ref,
    yfeat, xfeat, wvec, rows_all,
    halo_send, halo_recv, table_send, table_recv, fine_send, fine_recv, coarse_send, coarse_recv,
    rows_send, rows_recv, local_sem,
    *, caps,
):
    cap0, cap1 = caps
    leaf_dev, basis_rank, leaf_pts = basis_ref.shape
    vec_dev = sam_ref.shape[0]
    parents = leaf_dev // 2
    nb = farf_ref.shape[0] // leaf_dev
    nbc = farc_ref.shape[0] // parents
    nn = near_ref.shape[0] // leaf_dev
    devices, vecs = lax.axis_size("leaf"), lax.axis_size("vec")
    me, row = lax.axis_index("leaf"), lax.axis_index("vec")

    def leaf_peer(step):
        return {"leaf": lax.rem(me + step, devices)}

    def vec_peer(step):
        return {"vec": lax.rem(row + step, vecs)}

    def remote(src, dst, send, recv, peer):
        return pltpu.make_async_remote_copy(
            src_ref=src, dst_ref=dst, send_sem=send, recv_sem=recv,
            device_id=peer, device_id_type=MESH,
        )

    def cut(leaf):
        return pl.ds(pl.multiple_of(leaf * leaf_pts, leaf_pts), leaf_pts)

    def nt(a, b):
        return lax.dot_general(a, b, NT, preferred_element_type=jnp.float32)

    load_fine = pltpu.make_async_copy(cf_hbm, cf_ref, local_sem.at[0])
    load_coarse = pltpu.make_async_copy(cc_hbm, cc_ref, local_sem.at[1])
    load_fine.start()
    load_coarse.start()

    barrier = pltpu.get_barrier_semaphore()

    def greet(step, carry):
        pl.semaphore_signal(barrier, inc=1, device_id=leaf_peer(step), device_id_type=MESH)
        return carry

    lax.fori_loop(1, devices, greet, 0)
    for step in range(1, vecs):
        pl.semaphore_signal(barrier, inc=1, device_id=vec_peer(step), device_id_type=MESH)
    pl.semaphore_wait(barrier, devices - 1 + vecs - 1)

    def halos(side, geo_dst, sam_dst):
        peer = leaf_peer(1 if side == 0 else devices - 1)
        return (
            remote(geo_ref, geo_dst, halo_send.at[side, 0], halo_recv.at[side, 0], peer),
            remote(sam_ref, sam_dst, halo_send.at[side, 1], halo_recv.at[side, 1], peer),
        )

    @pl.when(me < devices - 1)
    def _():
        for copy in halos(0, geo_low, sam_low):
            copy.start()

    @pl.when(me > 0)
    def _():
        for copy in halos(1, geo_high, sam_high):
            copy.start()

    def table_copy(step):
        peer = lax.rem(me + step, devices)
        return remote(
            send_ref.at[peer], got.at[me], table_send.at[step], table_recv.at[step], {"leaf": peer}
        )

    def fine_copy(step):
        part = fine_all.at[pl.ds(me * leaf_dev, leaf_dev)]
        return remote(part, part, fine_send.at[step], fine_recv.at[step], leaf_peer(step))

    def coarse_copy(step):
        part = coarse_all.at[pl.ds(me * parents, parents)]
        return remote(part, part, coarse_send.at[step], coarse_recv.at[step], leaf_peer(step))

    def start_table(step, carry):
        table_copy(step).start()
        return carry

    lax.fori_loop(1, devices, start_table, 0)
    got[me] = send_ref[me]

    def fine_row(leaf, carry):
        coef = nt(sam_ref[:, cut(leaf)], basis_ref[leaf])
        fine_all[me * leaf_dev + leaf] = coef.astype(jnp.bfloat16)
        return carry

    lax.fori_loop(0, leaf_dev, fine_row, 0, unroll=4)

    def start_fine(step, carry):
        fine_copy(step).start()
        return carry

    lax.fori_loop(1, devices, start_fine, 0)

    def coarse_row(m, carry):
        child = me * leaf_dev + 2 * m
        coef = jnp.dot(fine_all[child], transfer_ref[m, 0], preferred_element_type=jnp.float32)
        coef += jnp.dot(fine_all[child + 1], transfer_ref[m, 1], preferred_element_type=jnp.float32)
        coarse_all[me * parents + m] = coef.astype(jnp.bfloat16)
        return carry

    lax.fori_loop(0, parents, coarse_row, 0, unroll=2)

    def start_coarse(step, carry):
        coarse_copy(step).start()
        return carry

    lax.fori_loop(1, devices, start_coarse, 0)

    def prepare(part, geo_src, sam_src):
        def source(leaf, carry):
            geo = geo_src[:, cut(leaf)]
            y1, y2, y3 = pieces(geo)
            rows = jnp.concatenate([y1, y1, y1, y2, y2, y3], axis=0)
            yfeat[part * leaf_dev + leaf] = rows.T.astype(jnp.bfloat16)
            scaled = sam_src[:, cut(leaf)].astype(jnp.float32) * geo[5:6]
            wvec[part * leaf_dev + leaf] = scaled.astype(jnp.bfloat16)
            return carry

        lax.fori_loop(0, leaf_dev, source, 0, unroll=4)

    prepare(1, geo_ref, sam_ref)

    def target(leaf, carry):
        xyz = geo_ref[0:3, cut(leaf)]
        norm = jnp.sum(xyz * xyz, axis=0, keepdims=True)
        x8 = jnp.concatenate(
            [-2.0 * xyz, jnp.ones_like(norm), norm, jnp.zeros_like(xyz)], axis=0
        )
        x1, x2, x3 = pieces(x8)
        xfeat[leaf] = jnp.concatenate([x1, x2, x3, x1, x2, x1], axis=0).astype(jnp.bfloat16)
        return carry

    lax.fori_loop(0, leaf_dev, target, 0, unroll=2)

    @pl.when(me > 0)
    def _():
        for copy in halos(0, geo_low, sam_low):
            copy.wait_recv()
        prepare(0, geo_low, sam_low)

    @pl.when(me < devices - 1)
    def _():
        for copy in halos(1, geo_high, sam_high):
            copy.wait_recv()
        prepare(2, geo_high, sam_high)

    def finish(step, carry):
        table_copy(step).wait()
        fine_copy(step).wait()
        coarse_copy(step).wait()
        return carry

    lax.fori_loop(1, devices, finish, 0)
    to_smem = pltpu.make_async_copy(got, got_smem, local_sem.at[2])
    to_smem.start()
    load_fine.wait()
    load_coarse.wait()
    to_smem.wait()

    def near_sum(leaf):
        features = xfeat[leaf]

        def step(group, total):
            for lane in range(4):
                chosen = near_ref[leaf * nn + group * 4 + lane]
                dist = jnp.dot(yfeat[chosen], features, preferred_element_type=jnp.float32)
                block = lax.rsqrt(dist.astype(jnp.bfloat16))
                total = total + jnp.dot(wvec[chosen], block, preferred_element_type=jnp.float32)
            return total

        zero = jnp.zeros((vec_dev, leaf_pts), jnp.float32)
        return lax.fori_loop(0, nn // 4, step, zero)

    def rows_copy(m, step):
        part = rows_all.at[row, :, pl.ds(pl.multiple_of(m * 2 * leaf_pts, 2 * leaf_pts), 2 * leaf_pts)]
        return remote(part, part, rows_send.at[step, m], rows_recv.at[step, m], vec_peer(step))

    def parent(m, carry):
        coarse = None
        for b in range(nbc):
            slot = farc_ref[m * nbc + b]
            source = lax.div(slot, cap1)
            index = source * parents + got_smem[source, 0, cap0 + lax.rem(slot, cap1)]
            term = nt(coarse_all[index], cc_ref[m, b])
            coarse = term if coarse is None else coarse + term
        coarse = coarse.astype(jnp.bfloat16)
        for s in range(2):
            leaf = 2 * m + s
            field = nt(coarse, transfer_ref[m, s])
            for b in range(nb):
                slot = farf_ref[leaf * nb + b]
                source = lax.div(slot, cap0)
                index = source * leaf_dev + got_smem[source, 0, lax.rem(slot, cap0)]
                field = field + nt(fine_all[index], cf_ref[leaf, b])
            local = field.astype(jnp.bfloat16)
            far = jnp.dot(local, basis_ref[leaf], preferred_element_type=jnp.float32)
            result = (near_sum(leaf) + far).astype(out_ref.dtype)
            rows_all[row, :, cut(leaf)] = result
            out_ref[:, cut(leaf)] = result
        for step in range(1, vecs):
            rows_copy(m, step).start()
        return carry

    lax.fori_loop(0, parents, parent, 0)

    @pl.when(me < devices - 1)
    def _():
        for copy in halos(0, geo_low, sam_low):
            copy.wait_send()

    @pl.when(me > 0)
    def _():
        for copy in halos(1, geo_high, sam_high):
            copy.wait_send()

    def gram_pair(m, carry):
        for step in range(1, vecs):
            rows_copy(m, step).wait()
        for s in range(2):
            leaf = 2 * m + s
            everyone = rows_all[:, :, cut(leaf)].reshape(vecs * vec_dev, leaf_pts)
            gram_ref[leaf] = nt(rows_all[row, :, cut(leaf)], everyone) * (1.0 / leaf_pts)
        return carry

    lax.fori_loop(0, parents, gram_pair, 0)


def per_device(
    samples, coords, panel_area, quad_weight, leaf_basis, transfer,
    coupling_fine, coupling_coarse, near_list, send_fine, send_coarse, far_fine, far_coarse,
):
    vec_dev, points = samples.shape
    leaf_dev, basis_rank, leaf_pts = leaf_basis.shape
    parents = leaf_dev // 2
    devices, vecs = lax.axis_size("leaf"), lax.axis_size("vec")
    device = lax.axis_index("leaf")
    caps = (send_fine.shape[1], send_coarse.shape[1])
    norm = jnp.sum(coords * coords, axis=0, keepdims=True) + panel_area[None, :]
    weight = quad_weight[None, :] / four_pi
    geo = jnp.concatenate(
        [coords, norm, jnp.ones_like(norm), weight, jnp.zeros((2, points), jnp.float32)], axis=0
    )
    window = (near_list - (device * leaf_dev - leaf_dev)).reshape(-1)
    send = jnp.concatenate([send_fine, send_coarse], axis=1)
    width = -(-send.shape[1] // 128) * 128
    send = jnp.pad(send, ((0, 0), (0, width - send.shape[1]))).reshape(devices, 1, width)
    smem = pl.BlockSpec(memory_space=pltpu.SMEM)
    vmem = pl.BlockSpec(memory_space=pltpu.VMEM)
    hbm = pl.BlockSpec(memory_space=pl.ANY)
    bf16 = jnp.bfloat16
    dma = pltpu.SemaphoreType.DMA
    sample_out, gram = pl.pallas_call(
        functools.partial(main_kernel, caps=caps),
        out_shape=(
            jax.ShapeDtypeStruct((vec_dev, points), bf16),
            jax.ShapeDtypeStruct((leaf_dev, vec_dev, vecs * vec_dev), jnp.float32),
        ),
        in_specs=[smem] * 3 + [vmem] * 5 + [hbm] * 2,
        out_specs=(vmem, vmem),
        scratch_shapes=[
            pltpu.VMEM(geo.shape, jnp.float32),
            pltpu.VMEM(geo.shape, jnp.float32),
            pltpu.VMEM(samples.shape, bf16),
            pltpu.VMEM(samples.shape, bf16),
            pltpu.VMEM((devices * leaf_dev, vec_dev, basis_rank), bf16),
            pltpu.VMEM((devices * parents, vec_dev, basis_rank), bf16),
            pltpu.VMEM(send.shape, jnp.int32),
            pltpu.SMEM(send.shape, jnp.int32),
            pltpu.VMEM(coupling_fine.shape, bf16),
            pltpu.VMEM(coupling_coarse.shape, bf16),
            pltpu.VMEM((3 * leaf_dev, leaf_pts, 48), bf16),
            pltpu.VMEM((leaf_dev, 48, leaf_pts), bf16),
            pltpu.VMEM((3 * leaf_dev, vec_dev, leaf_pts), bf16),
            pltpu.VMEM((vecs, vec_dev, points), bf16),
            dma((2, 2)), dma((2, 2)),
            dma((devices,)), dma((devices,)),
            dma((devices,)), dma((devices,)),
            dma((devices,)), dma((devices,)),
            dma((vecs, parents)), dma((vecs, parents)),
            dma((3,)),
        ],
        compiler_params=pltpu.CompilerParams(
            vmem_limit_bytes=56 * 1024 * 1024, collective_id=0, has_side_effects=True
        ),
    )(
        window, far_fine.reshape(-1), far_coarse.reshape(-1),
        geo, samples, send, transfer, leaf_basis, coupling_fine, coupling_coarse,
    )
    return sample_out, gram


def solution(mesh):
    return jax.shard_map(
        per_device,
        mesh=mesh,
        in_specs=(
            P("vec", "leaf"), P(None, "leaf"), P("leaf"), P("leaf"),
            P("leaf", None, None), P("leaf", None, None, None),
            P("leaf", None, None, None), P("leaf", None, None, None),
            P("leaf", None), P("leaf", None), P("leaf", None), P("leaf", None), P("leaf", None),
        ),
        out_specs=(P("vec", "leaf"), P("leaf", "vec", None)),
        check_vma=False,
    )
```

```python
import functools
import jax
import jax.numpy as jnp
from jax import lax
from jax.experimental import pallas as pl
from jax.experimental.pallas import tpu as pltpu
from jax.sharding import PartitionSpec as P

four_pi = 4.0 * 3.141592653589793
NT = (((1,), (1,)), ((), ()))
MESH = pl.DeviceIdType.MESH


def pieces(block):
    first = block.astype(jnp.bfloat16).astype(jnp.float32)
    rest = block - first
    second = rest.astype(jnp.bfloat16).astype(jnp.float32)
    return first, second, rest - second


def main_kernel(
    near_ref, farf_ref, farc_ref,
    coords_ref, area_ref, weight_ref, sam_ref, send_ref, transfer_ref, basis_ref, cf_hbm, cc_hbm,
    out_ref, gram_ref,
    geo_ref, near_all, geo_low, geo_high, sam_low, sam_high, fine_all, coarse_all, got, got_smem, cf_ref, cc_ref,
    yfeat, xfeat, wvec, rows_all,
    halo_send, halo_recv, table_send, table_recv, fine_send, fine_recv, coarse_send, coarse_recv,
    rows_send, rows_recv, local_sem,
    *, caps,
):
    cap0, cap1 = caps
    leaf_dev, basis_rank, leaf_pts = basis_ref.shape
    vec_dev = sam_ref.shape[0]
    parents = leaf_dev // 2
    nb = farf_ref.shape[1]
    nbc = farc_ref.shape[1]
    nn = near_ref.shape[1]
    devices, vecs = lax.axis_size("leaf"), lax.axis_size("vec")
    me, row = lax.axis_index("leaf"), lax.axis_index("vec")

    def leaf_peer(step):
        return {"leaf": lax.rem(me + step, devices)}

    def vec_peer(step):
        return {"vec": lax.rem(row + step, vecs)}

    def remote(src, dst, send, recv, peer):
        return pltpu.make_async_remote_copy(
            src_ref=src, dst_ref=dst, send_sem=send, recv_sem=recv,
            device_id=peer, device_id_type=MESH,
        )

    def cut(leaf):
        return pl.ds(pl.multiple_of(leaf * leaf_pts, leaf_pts), leaf_pts)

    def nt(a, b):
        return lax.dot_general(a, b, NT, preferred_element_type=jnp.float32)

    load_fine = pltpu.make_async_copy(cf_hbm, cf_ref, local_sem.at[0])
    load_coarse = pltpu.make_async_copy(cc_hbm, cc_ref, local_sem.at[1])
    load_fine.start()
    load_coarse.start()

    def geometry(leaf, carry):
        xyz = coords_ref[:, cut(leaf)]
        norm = jnp.sum(xyz * xyz, axis=0, keepdims=True) + area_ref[:, cut(leaf)]
        weight = weight_ref[:, cut(leaf)] * (1.0 / four_pi)
        geo_ref[:, cut(leaf)] = jnp.concatenate(
            [xyz, norm, jnp.ones_like(norm), weight, jnp.zeros_like(xyz[:2])], axis=0
        )
        return carry

    lax.fori_loop(0, leaf_dev, geometry, 0, unroll=4)
    barrier = pltpu.get_barrier_semaphore()

    def greet(step, carry):
        pl.semaphore_signal(barrier, inc=1, device_id=leaf_peer(step), device_id_type=MESH)
        return carry

    lax.fori_loop(1, devices, greet, 0)
    for step in range(1, vecs):
        pl.semaphore_signal(barrier, inc=1, device_id=vec_peer(step), device_id_type=MESH)
    pl.semaphore_wait(barrier, devices - 1 + vecs - 1)

    def halos(side, geo_dst, sam_dst):
        peer = leaf_peer(1 if side == 0 else devices - 1)
        return (
            remote(geo_ref, geo_dst, halo_send.at[side, 0], halo_recv.at[side, 0], peer),
            remote(sam_ref, sam_dst, halo_send.at[side, 1], halo_recv.at[side, 1], peer),
        )

    @pl.when(me < devices - 1)
    def _():
        for copy in halos(0, geo_low, sam_low):
            copy.start()

    @pl.when(me > 0)
    def _():
        for copy in halos(1, geo_high, sam_high):
            copy.start()

    def table_copy(step):
        peer = lax.rem(me + step, devices)
        return remote(
            send_ref.at[peer], got.at[me], table_send.at[step], table_recv.at[step], {"leaf": peer}
        )

    def fine_copy(step):
        part = fine_all.at[pl.ds(me * leaf_dev, leaf_dev)]
        return remote(part, part, fine_send.at[step], fine_recv.at[step], leaf_peer(step))

    def coarse_copy(step):
        part = coarse_all.at[pl.ds(me * parents, parents)]
        return remote(part, part, coarse_send.at[step], coarse_recv.at[step], leaf_peer(step))

    def start_table(step, carry):
        table_copy(step).start()
        return carry

    lax.fori_loop(1, devices, start_table, 0)
    got[me] = send_ref[me]

    def fine_row(leaf, carry):
        coef = nt(sam_ref[:, cut(leaf)], basis_ref[leaf])
        fine_all[me * leaf_dev + leaf] = coef.astype(jnp.bfloat16)
        return carry

    lax.fori_loop(0, leaf_dev, fine_row, 0, unroll=4)

    def coarse_row(m, carry):
        child = me * leaf_dev + 2 * m
        coef = jnp.dot(fine_all[child], transfer_ref[m, 0], preferred_element_type=jnp.float32)
        coef += jnp.dot(fine_all[child + 1], transfer_ref[m, 1], preferred_element_type=jnp.float32)
        coarse_all[me * parents + m] = coef.astype(jnp.bfloat16)
        return carry

    lax.fori_loop(0, parents, coarse_row, 0, unroll=2)

    def prepare(part, geo_src, sam_src):
        def source(leaf, carry):
            geo = geo_src[:, cut(leaf)]
            y1, y2, y3 = pieces(geo)
            rows = jnp.concatenate([y1, y1, y1, y2, y2, y3], axis=0)
            yfeat[part * leaf_dev + leaf] = rows.T.astype(jnp.bfloat16)
            scaled = sam_src[:, cut(leaf)].astype(jnp.float32) * geo[5:6]
            wvec[part * leaf_dev + leaf] = scaled.astype(jnp.bfloat16)
            return carry

        lax.fori_loop(0, leaf_dev, source, 0, unroll=4)

    prepare(1, geo_ref, sam_ref)

    def target(leaf, carry):
        xyz = geo_ref[0:3, cut(leaf)]
        norm = jnp.sum(xyz * xyz, axis=0, keepdims=True)
        x8 = jnp.concatenate(
            [-2.0 * xyz, jnp.ones_like(norm), norm, jnp.zeros_like(xyz)], axis=0
        )
        x1, x2, x3 = pieces(x8)
        xfeat[leaf] = jnp.concatenate([x1, x2, x3, x1, x2, x1], axis=0).astype(jnp.bfloat16)
        return carry

    lax.fori_loop(0, leaf_dev, target, 0, unroll=2)

    @pl.when(me > 0)
    def _():
        for copy in halos(0, geo_low, sam_low):
            copy.wait_recv()
        prepare(0, geo_low, sam_low)

    @pl.when(me < devices - 1)
    def _():
        for copy in halos(1, geo_high, sam_high):
            copy.wait_recv()
        prepare(2, geo_high, sam_high)

    def start_fine(step, carry):
        fine_copy(step).start()
        return carry

    lax.fori_loop(1, devices, start_fine, 0)

    def start_coarse(step, carry):
        coarse_copy(step).start()
        return carry

    lax.fori_loop(1, devices, start_coarse, 0)

    def near_sum(leaf):
        features = xfeat[leaf]

        def step(group, total):
            for lane in range(4):
                offset = near_ref[leaf, group * 4 + lane] - (me - 1) * leaf_dev
                chosen = jnp.clip(offset, 0, 3 * leaf_dev - 1)
                dist = jnp.dot(yfeat[chosen], features, preferred_element_type=jnp.float32)
                block = lax.rsqrt(dist.astype(jnp.bfloat16))
                total = total + jnp.dot(wvec[chosen], block, preferred_element_type=jnp.float32)
            return total

        zero = jnp.zeros((vec_dev, leaf_pts), jnp.float32)
        return lax.fori_loop(0, nn // 4, step, zero)

    def near_leaf(leaf, carry):
        near_all[leaf] = near_sum(leaf)
        return carry

    lax.fori_loop(0, leaf_dev, near_leaf, 0)

    def finish(step, carry):
        table_copy(step).wait()
        fine_copy(step).wait()
        coarse_copy(step).wait()
        return carry

    lax.fori_loop(1, devices, finish, 0)
    to_smem = pltpu.make_async_copy(got, got_smem, local_sem.at[2])
    to_smem.start()
    load_fine.wait()
    load_coarse.wait()
    to_smem.wait()

    def rows_copy(m, step):
        part = rows_all.at[row, :, pl.ds(pl.multiple_of(m * 2 * leaf_pts, 2 * leaf_pts), 2 * leaf_pts)]
        return remote(part, part, rows_send.at[step, m], rows_recv.at[step, m], vec_peer(step))

    def parent(m, carry):
        coarse = None
        for b in range(nbc):
            slot = farc_ref[m, b]
            source = lax.div(slot, cap1)
            index = source * parents + got_smem[source, 0, cap0 + lax.rem(slot, cap1)]
            term = nt(coarse_all[index], cc_ref[m, b])
            coarse = term if coarse is None else coarse + term
        coarse = coarse.astype(jnp.bfloat16)
        for s in range(2):
            leaf = 2 * m + s
            field = nt(coarse, transfer_ref[m, s])
            for b in range(nb):
                slot = farf_ref[leaf, b]
                source = lax.div(slot, cap0)
                index = source * leaf_dev + got_smem[source, 0, lax.rem(slot, cap0)]
                field = field + nt(fine_all[index], cf_ref[leaf, b])
            local = field.astype(jnp.bfloat16)
            far = jnp.dot(local, basis_ref[leaf], preferred_element_type=jnp.float32)
            result = (near_all[leaf] + far).astype(out_ref.dtype)
            rows_all[row, :, cut(leaf)] = result
            out_ref[:, cut(leaf)] = result
        for step in range(1, vecs):
            rows_copy(m, step).start()
        return carry

    lax.fori_loop(0, parents, parent, 0)

    @pl.when(me < devices - 1)
    def _():
        for copy in halos(0, geo_low, sam_low):
            copy.wait_send()

    @pl.when(me > 0)
    def _():
        for copy in halos(1, geo_high, sam_high):
            copy.wait_send()

    def gram_pair(m, carry):
        for step in range(1, vecs):
            rows_copy(m, step).wait()
        for s in range(2):
            leaf = 2 * m + s
            everyone = rows_all[:, :, cut(leaf)].reshape(vecs * vec_dev, leaf_pts)
            gram_ref[leaf] = nt(rows_all[row, :, cut(leaf)], everyone) * (1.0 / leaf_pts)
        return carry

    lax.fori_loop(0, parents, gram_pair, 0)


def per_device(
    samples, coords, panel_area, quad_weight, leaf_basis, transfer,
    coupling_fine, coupling_coarse, near_list, send_fine, send_coarse, far_fine, far_coarse,
):
    vec_dev, points = samples.shape
    leaf_dev, basis_rank, leaf_pts = leaf_basis.shape
    parents = leaf_dev // 2
    devices, vecs = lax.axis_size("leaf"), lax.axis_size("vec")
    caps = (send_fine.shape[1], send_coarse.shape[1])
    send = jnp.concatenate([send_fine, send_coarse], axis=1)
    width = -(-send.shape[1] // 128) * 128
    send = jnp.pad(send, ((0, 0), (0, width - send.shape[1]))).reshape(devices, 1, width)
    smem = pl.BlockSpec(memory_space=pltpu.SMEM)
    vmem = pl.BlockSpec(memory_space=pltpu.VMEM)
    hbm = pl.BlockSpec(memory_space=pl.ANY)
    bf16 = jnp.bfloat16
    dma = pltpu.SemaphoreType.DMA
    sample_out, gram = pl.pallas_call(
        functools.partial(main_kernel, caps=caps),
        out_shape=(
            jax.ShapeDtypeStruct((vec_dev, points), bf16),
            jax.ShapeDtypeStruct((leaf_dev, vec_dev, vecs * vec_dev), jnp.float32),
        ),
        in_specs=[smem] * 3 + [vmem] * 7 + [hbm] * 2,
        out_specs=(vmem, vmem),
        scratch_shapes=[
            pltpu.VMEM((8, points), jnp.float32),
            pltpu.VMEM((leaf_dev, vec_dev, leaf_pts), jnp.float32),
            pltpu.VMEM((8, points), jnp.float32),
            pltpu.VMEM((8, points), jnp.float32),
            pltpu.VMEM(samples.shape, bf16),
            pltpu.VMEM(samples.shape, bf16),
            pltpu.VMEM((devices * leaf_dev, vec_dev, basis_rank), bf16),
            pltpu.VMEM((devices * parents, vec_dev, basis_rank), bf16),
            pltpu.VMEM(send.shape, jnp.int32),
            pltpu.SMEM(send.shape, jnp.int32),
            pltpu.VMEM(coupling_fine.shape, bf16),
            pltpu.VMEM(coupling_coarse.shape, bf16),
            pltpu.VMEM((3 * leaf_dev, leaf_pts, 48), bf16),
            pltpu.VMEM((leaf_dev, 48, leaf_pts), bf16),
            pltpu.VMEM((3 * leaf_dev, vec_dev, leaf_pts), bf16),
            pltpu.VMEM((vecs, vec_dev, points), bf16),
            dma((2, 2)), dma((2, 2)),
            dma((devices,)), dma((devices,)),
            dma((devices,)), dma((devices,)),
            dma((devices,)), dma((devices,)),
            dma((vecs, parents)), dma((vecs, parents)),
            dma((3,)),
        ],
        compiler_params=pltpu.CompilerParams(
            vmem_limit_bytes=56 * 1024 * 1024, collective_id=0, has_side_effects=True
        ),
    )(
        near_list, far_fine, far_coarse,
        coords, panel_area[None, :], quad_weight[None, :], samples, send, transfer, leaf_basis, coupling_fine, coupling_coarse,
    )
    return sample_out, gram


def solution(mesh):
    return jax.shard_map(
        per_device,
        mesh=mesh,
        in_specs=(
            P("vec", "leaf"), P(None, "leaf"), P("leaf"), P("leaf"),
            P("leaf", None, None), P("leaf", None, None, None),
            P("leaf", None, None, None), P("leaf", None, None, None),
            P("leaf", None), P("leaf", None), P("leaf", None), P("leaf", None), P("leaf", None),
        ),
        out_specs=(P("vec", "leaf"), P("leaf", "vec", None)),
        check_vma=False,
    )
```
